32 devices in a mesh: dp: 2 (over x), mode: 4 (over z), tm: 4 (over y, core).
Axes of the slice: x: 2, y: 2, z: 4, core: 2. Of those that a mesh axis runs over, the one named last changes fastest.
Arguments:
- input_field: float32 [2, 16, 8, 16384], P(None, 'dp', 'mode', 'tm'), parts along dimension 1, may hold values from -6 to 6
- target_field: float32 [2, 16, 8, 16384], P(None, 'dp', 'mode', 'tm'), parts along dimension 1, may hold values from -6 to 6
- margin: float32 [8, 8, 16], P('mode'), may hold values from -0.5 to 0.5
- pair_index: int32 [16, 2], replicated, may hold values from 0 to 7
- mode_beta: float32 [1024, 8, 3], P(None, 'mode'), may hold values from -2 to 2
- segment_kind: int32 [1], replicated, may hold values from 0 to 1023
Outputs:
- field_gradient: float32 [2, 16, 8, 16384], P(None, 'dp', 'mode', 'tm'), parts along dimension 1
The draws below stay inside these ranges and needn't reach their ends.
There are 2 independent parts, one for each index of `dp`. The reference program is written for one: setup_inputs(seed, part) draws one part's arguments, and reference() takes and returns one part's arrays. A program takes and returns all parts, laid end to end along the dimension named above; an argument that names none is the same for every part. Nothing has to cross between parts.
All inputs are finite; a program needn't handle non-finite values.
Results may differ from the reference program's by a relative error of at most 0.00011.
Values sent between devices are 32-bit elements; how exact they have to be, the bound alone decides.
A program may use at most 128 MiB of HBM per device.

```python
import jax
import jax.numpy as jnp
from jax import lax

PULSES = 8
NT = 16384
PAIRS = 16
STEPS = 1
KINDS = 1024
MODES = 8


def set_ends(array, own_key, low, largest):
    spot = [jax.random.randint(jax.random.fold_in(own_key, axis), (), 0, length) for axis, length in enumerate(array.shape)]
    widest = array.shape.index(max(array.shape))
    neighbour = spot[:widest] + [(spot[widest] + 1) % array.shape[widest]] + spot[widest + 1:]
    return array.at[tuple(spot)].set(low).at[tuple(neighbour)].set(largest)


def steps_of(rng, dims, split, low, high):
    factor_of, own = 1.0, jax.random.fold_in(rng, 6)
    for dim, blocks in split:
        heights = jnp.exp(jax.random.uniform(jax.random.fold_in(own, dim), (blocks,), jnp.float32, low / len(split), high / len(split)))
        factor_of = factor_of * jnp.repeat(heights, dims[dim] // blocks).reshape([-1 if axis == dim else 1 for axis in range(len(dims))])
    return factor_of


def normal_values(stream_key, shape, spread, most, shards=(), kind=jnp.bfloat16):
    drawn = jax.random.normal(stream_key, shape, jnp.float32) * spread
    if len(shards) > 0:
        drawn = steps_of(stream_key, shape, shards, -0.22, 0.18) * drawn
    return jnp.clip(drawn, min=-most, max=most).astype(kind)


def setup_inputs(seed: int = 0, part: int = 0) -> dict:
    key_list = jax.random.split(jax.random.key(seed), 7)
    own_keys = jax.random.split(jax.random.fold_in(key_list[6], part), 7)
    input_field = normal_values(own_keys[0], (2, PULSES, MODES, NT), 1.0, 6.0, ((2, 4), (3, 4)), jnp.float32)
    target_field = normal_values(own_keys[1], (2, PULSES, MODES, NT), 1.0, 6.0, ((2, 4), (3, 4)), jnp.float32)
    margin = normal_values(key_list[2], (MODES, MODES, PAIRS), (MODES * PAIRS) ** -0.5, 0.5, ((0, 4),), jnp.float32)
    pair_index = set_ends(jax.random.randint(key_list[3], (PAIRS, 2), 0, MODES), jax.random.fold_in(key_list[3], 1), 0, MODES - 1).astype(jnp.int32)
    mode_beta = jnp.clip(jax.random.uniform(key_list[4], (KINDS, MODES, 3), jnp.float32, -2.0, 2.0) * steps_of(key_list[4], (KINDS, MODES, 3), ((1, 4),), -0.4, 0.0), -2.0, 2.0)
    segment_kind = jax.random.randint(key_list[5], (STEPS,), 0, KINDS).astype(jnp.int32)
    return dict(input_field=input_field, target_field=target_field, margin=margin, pair_index=pair_index, mode_beta=mode_beta, segment_kind=segment_kind)


kerr_scale = 0.1

def phases(mode_table):
    index = jnp.arange(NT, dtype=jnp.int32)
    signed = jnp.where(index < NT // 2, index, index - NT).astype(jnp.float32)
    omega = signed * (8.0 / NT)
    return mode_table[:, 0:1] * omega + mode_table[:, 1:2] * omega ** 2 / 2.0 + mode_table[:, 2:3] * omega ** 3 / 6.0

def disperse(pulse_field, phase):
    values = pulse_field[0] + 1j * pulse_field[1]
    spectrum = jnp.fft.fft(values, axis=-1) * jnp.exp(1j * phase)[None]
    result = jnp.fft.ifft(spectrum, axis=-1)
    return jnp.stack([jnp.real(result), jnp.imag(result)])

def nonlinear(pulse_field, margin, pair_index):

    def single(pulse):
        left = pulse[:, pair_index[:, 0], :]
        right = pulse[:, pair_index[:, 1], :]
        prod_real = left[0] * right[0] - left[1] * right[1]
        prod_imag = left[0] * right[1] + left[1] * right[0]
        coup_real = jnp.einsum('pnj,js->pns', margin, prod_real, precision=lax.Precision.HIGHEST)
        coup_imag = jnp.einsum('pnj,js->pns', margin, prod_imag, precision=lax.Precision.HIGHEST)
        non_real = lax.optimization_barrier(jnp.sum(coup_real * pulse[0][None] + coup_imag * pulse[1][None], axis=1))
        non_imag = lax.optimization_barrier(jnp.sum(coup_imag * pulse[0][None] - coup_real * pulse[1][None], axis=1))
        return jnp.stack([-kerr_scale * non_imag, kerr_scale * non_real])
    mapped = lax.map(single, jnp.moveaxis(pulse_field, 1, 0))
    return jnp.moveaxis(mapped, 0, 1)

def forward(pulse_field, margin, pair_index, mode_beta, segment_kind):
    for segment in range(STEPS):
        phase = phases(mode_beta[segment_kind[segment]])
        pulse_field = disperse(pulse_field, phase)
        pulse_field = pulse_field + nonlinear(pulse_field, margin, pair_index)
    return pulse_field

def reference(input_field, target_field, margin, pair_index, mode_beta, segment_kind):

    def misfit(pulse_field):
        output_field = forward(pulse_field, margin, pair_index, mode_beta, segment_kind)
        return jnp.sum((output_field - target_field) ** 2)
    value, pullback = jax.vjp(misfit, input_field)
    gradient = pullback(jnp.ones_like(value))[0]
    return gradient
```

```python
import functools
import math

import jax
import jax.numpy as jnp
import numpy as np
from jax import lax
from jax.experimental import pallas as pl
from jax.experimental.pallas import tpu as pltpu
from jax.sharding import PartitionSpec as P

kerr_scale = 0.1
MESH = pl.DeviceIdType.MESH
f32 = jnp.float32
bf16 = jnp.bfloat16


def split_table(table):
    high = table.astype(np.float32).astype(bf16)
    low = (table - high.astype(np.float64)).astype(np.float32).astype(bf16)
    return np.stack([np.asarray(high), np.asarray(low)])


def real_form(size):
    turns = np.outer(np.arange(size), np.arange(size)) % size
    angle = turns * (2.0 * math.pi / size)
    cosine, sine = np.cos(angle), np.sin(angle)
    return np.block([[cosine, sine], [-sine, cosine]])


def make_tables(outer, total):
    left, right = real_form(outer), real_form(128)
    turns = np.outer(np.arange(outer), np.arange(128)) % total
    angle = turns * (2.0 * math.pi / total)
    twist = np.stack([np.cos(angle), -np.sin(angle)]).astype(np.float32)
    return (
        split_table(left),
        split_table(left.T / total),
        split_table(right.T),
        split_table(right),
        twist,
    )


def halves(value):
    high = value.astype(bf16)
    return high, (value - high.astype(f32)).astype(bf16)


def mm(a, b):
    return jnp.dot(a, b, preferred_element_type=f32)


def left_dot(table, value):
    high, low = halves(value)
    return mm(table[0], high) + (mm(table[0], low) + mm(table[1], high))


def right_dot(value, table):
    high, low = halves(value)
    return mm(high, table[0]) + (mm(low, table[0]) + mm(high, table[1]))


def kernel(
    sizes, coeffs, pairs, one_left, one_right, x, target, margin,
    left_f_hbm, left_i_hbm, right_f_hbm, right_i_hbm, twist_hbm, out,
    left_f, left_i, right_f, right_i, twist, phase_tab,
    rows_in, send_z, kb, t1, t2, mg, mg_s, prods, coup, grad_pair, moved, cots, grads, rows_back, send_out,
    table_sem, own_sem, in_s, in_r, mg_ss, mg_r, t1_s, t1_r, t2_s, t2_r, kb_s, kb_r, gb_s, gb_r, out_s, out_r,
):
    Dt, Dm, B, Bl, ml, M, A, Al, As, Ak, J, total = sizes
    me_t = lax.axis_index("tm")
    me_m = lax.axis_index("mode")
    tm_peers = [lax.rem(me_t + d, Dt) for d in range(1, Dt)]
    mode_peers = [lax.rem(me_m + d, Dm) for d in range(1, Dm)]

    def remote(src, dst, send, recv, axis, peer):
        return pltpu.make_async_remote_copy(
            src_ref=src, dst_ref=dst, send_sem=send, recv_sem=recv, device_id={axis: peer}, device_id_type=MESH
        )

    barrier = pltpu.get_barrier_semaphore()
    for peer in tm_peers:
        pl.semaphore_signal(barrier, inc=1, device_id={"tm": peer}, device_id_type=MESH)
    for peer in mode_peers:
        pl.semaphore_signal(barrier, inc=1, device_id={"mode": peer}, device_id_type=MESH)
    pl.semaphore_wait(barrier, Dt + Dm - 2)

    sends = []
    owns = {}
    own_count = [0]

    def go(src, dst, send, recv, axis, peer):
        copy = remote(src, dst, send, recv, axis, peer)
        copy.start()
        sends.append(copy)

    def own(name, src, dst):
        copy = pltpu.make_async_copy(src, dst, own_sem.at[own_count[0]])
        own_count[0] += 1
        copy.start()
        owns[name] = copy

    def target_part(i):
        if (As * ml) % 8 == 0:
            return target.at[:, :, pl.ds(pl.multiple_of(i * (As * ml), 8), As * ml), :]
        return target.at[i]

    for b in range(Bl):
        for peer in tm_peers:
            go(x.at[:, peer * Bl + b], rows_in.at[b, me_t], in_s.at[b, peer], in_r.at[b, me_t], "tm", peer)
        own(("in", b), x.at[:, me_t * Bl + b], rows_in.at[b, me_t])
    for peer in mode_peers:
        go(margin, mg.at[me_m], mg_ss.at[peer], mg_r.at[me_m], "mode", peer)
    own("mg", margin, mg.at[me_m])
    for peer in mode_peers:
        go(target_part(peer), t1.at[me_m], t1_s.at[peer], t1_r.at[me_m], "mode", peer)
    own("t1", target_part(me_m), t1.at[me_m])
    table_copies = []
    for spot, (src, dst) in enumerate(
        ((left_f_hbm, left_f), (left_i_hbm, left_i), (right_f_hbm, right_f), (right_i_hbm, right_i), (twist_hbm, twist))
    ):
        copy = pltpu.make_async_copy(src, dst, table_sem.at[spot])
        copy.start()
        table_copies.append(copy)

    low_digit = lax.broadcasted_iota(jnp.int32, (A, 128), 0)
    high_digit = lax.broadcasted_iota(jnp.int32, (A, 128), 1)
    frequency = low_digit + A * high_digit
    signed = jnp.where(frequency < total // 2, frequency, frequency - total).astype(f32)
    omega = signed * (8.0 / total)
    for m in range(ml):
        phase = (
            coeffs[m, 0] * omega + coeffs[m, 1] * (omega * omega) / 2.0 + coeffs[m, 2] * (omega * omega * omega) / 6.0
        )
        phase_tab[0, m * A : (m + 1) * A, :] = jnp.cos(phase)
        phase_tab[1, m * A : (m + 1) * A, :] = jnp.sin(phase)
    for copy in table_copies:
        copy.wait()

    def disperse(stacked, direction):
        spun = left_dot(left_f, stacked)
        tw_r, tw_i = twist[0], twist[1]
        blocks = []
        for m in range(ml):
            re = spun[:A, m * 128 : (m + 1) * 128]
            im = spun[A:, m * 128 : (m + 1) * 128]
            blocks.append(jnp.concatenate([re * tw_r - im * tw_i, re * tw_i + im * tw_r], axis=1))
        spectrum = right_dot(jnp.concatenate(blocks, axis=0), right_f)
        re, im = spectrum[:, :128], spectrum[:, 128:]
        cosine = phase_tab[0]
        sine = phase_tab[1] * direction
        turned = jnp.concatenate([re * cosine - im * sine, re * sine + im * cosine], axis=1)
        back = right_dot(turned, right_i)
        real_rows, imag_rows = [], []
        for m in range(ml):
            re = back[m * A : (m + 1) * A, :128]
            im = back[m * A : (m + 1) * A, 128:]
            real_rows.append(re * tw_r + im * tw_i)
            imag_rows.append(im * tw_r - re * tw_i)
        joined = jnp.concatenate(
            [jnp.concatenate(real_rows, axis=1), jnp.concatenate(imag_rows, axis=1)], axis=0
        )
        return left_dot(left_i, joined)

    for b in range(Bl):
        owns[("in", b)].wait()
        for peer in tm_peers:
            remote(x.at[:, b], rows_in.at[b, peer], in_s.at[b, peer], in_r.at[b, peer], "tm", peer).wait_recv()
        stacked = jnp.concatenate(
            [
                jnp.concatenate(
                    [rows_in[b, j, ri, pl.ds(m, Al, stride=ml), :] for ri in range(2) for j in range(Dt)], axis=0
                )
                for m in range(ml)
            ],
            axis=1,
        )
        result = disperse(stacked, 1.0)
        for i in range(Dm):
            for m in range(ml):
                for ri in range(2):
                    for j in range(Dt):
                        row = ri * A + j * Al + i * As
                        send_z[i, b, m, ri, j * As : (j + 1) * As, :] = result[row : row + As, m * 128 : (m + 1) * 128]
        for peer in mode_peers:
            go(send_z.at[peer, b], kb[b].at[pl.ds(me_m * ml, ml)], kb_s.at[b, peer], kb_r.at[b, me_m], "mode", peer)
        own(("kb", b), send_z.at[me_m, b], kb[b].at[pl.ds(me_m * ml, ml)])

    owns["t1"].wait()
    for peer in mode_peers:
        remote(target_part(0), t1.at[peer], t1_s.at[peer], t1_r.at[peer], "mode", peer).wait_recv()
    for peer in tm_peers:
        go(t1.at[:, :, pl.ds(peer * Bl, Bl)], t2.at[me_t], t2_s.at[peer], t2_r.at[me_t], "tm", peer)
    own("t2", t1.at[:, :, pl.ds(me_t * Bl, Bl)], t2.at[me_t])
    owns["mg"].wait()
    for peer in mode_peers:
        remote(margin, mg.at[peer], mg_ss.at[peer], mg_r.at[peer], "mode", peer).wait_recv()
    own("mgs", mg, mg_s)
    owns["mgs"].wait()
    owns["t2"].wait()
    for peer in tm_peers:
        remote(
            t1.at[:, :, pl.ds(0, Bl)], t2.at[peer], t2_s.at[peer], t2_r.at[peer], "tm", peer
        ).wait_recv()

    zero = jnp.zeros((Ak, 128), f32)

    def weight(p, n, j):
        return mg_s[p // ml, lax.rem(p, ml), n * J + j]

    for b in range(Bl):
        owns[("kb", b)].wait()
        for peer in mode_peers:
            remote(
                send_z.at[0, b], kb[b].at[pl.ds(peer * ml, ml)], kb_s.at[b, peer], kb_r.at[b, peer], "mode", peer
            ).wait_recv()

        @pl.loop(0, J)
        def _(j):
            first, second = pairs[j, 0], pairs[j, 1]
            ar, ai = kb[b][first, 0], kb[b][first, 1]
            br, bi = kb[b][second, 0], kb[b][second, 1]
            prods[j, 0] = ar * br - ai * bi
            prods[j, 1] = ar * bi + ai * br

        @pl.loop(0, M)
        def _(p):
            def inner(step, carry):
                kr, ki = carry
                sums = [zero] * 4
                for j in range(J):
                    pr, pi = prods[j, 0], prods[j, 1]
                    for s in range(2):
                        w = weight(p, step * 2 + s, j)
                        sums[2 * s] = sums[2 * s] + w * pr
                        sums[2 * s + 1] = sums[2 * s + 1] + w * pi
                for s in range(2):
                    n = step * 2 + s
                    cr, ci = sums[2 * s], sums[2 * s + 1]
                    coup[p * M + n, 0] = cr
                    coup[p * M + n, 1] = ci
                    ur, ui = kb[b][n, 0], kb[b][n, 1]
                    kr = kr + (cr * ur + ci * ui)
                    ki = ki + (ci * ur - cr * ui)
                return kr, ki

            kr, ki = lax.fori_loop(0, M // 2, inner, (zero, zero))
            owner, local = p // ml, lax.rem(p, ml)
            wanted = [
                jnp.concatenate(
                    [t2[j, owner, ri, b, pl.ds(local, As, stride=ml), :] for j in range(Dt)], axis=0
                )
                for ri in range(2)
            ]
            cots[p, 0] = 2.0 * (kb[b][p, 0] - kerr_scale * ki - wanted[0])
            cots[p, 1] = 2.0 * (kb[b][p, 1] + kerr_scale * kr - wanted[1])

        @pl.loop(0, M)
        def _(n):
            ur, ui = kb[b][n, 0], kb[b][n, 1]

            def inner(p, carry):
                gr, gi = carry
                er, ei = kerr_scale * cots[p, 1], -kerr_scale * cots[p, 0]
                cr, ci = coup[p * M + n, 0], coup[p * M + n, 1]
                gr = gr + (er * cr + ei * ci)
                gi = gi + (er * ci - ei * cr)
                coup[p * M + n, 0] = er * ur - ei * ui
                coup[p * M + n, 1] = er * ui + ei * ur
                return gr, gi

            gr, gi = lax.fori_loop(0, M, inner, (cots[n, 0], cots[n, 1]))
            grads[b, n, 0] = gr
            grads[b, n, 1] = gi

        @pl.loop(0, J // 4)
        def _(quad):
            def outer(p, carry):
                sums = list(carry)
                for n in range(M):
                    sr, si = coup[p * M + n, 0], coup[p * M + n, 1]
                    for s in range(4):
                        w = weight(p, n, quad * 4 + s)
                        sums[2 * s] = sums[2 * s] + w * sr
                        sums[2 * s + 1] = sums[2 * s + 1] + w * si
                return tuple(sums)

            sums = lax.fori_loop(0, M, outer, (zero,) * 8)
            for s in range(4):
                grad_pair[quad * 4 + s, 0] = sums[2 * s]
                grad_pair[quad * 4 + s, 1] = sums[2 * s + 1]

        @pl.loop(0, J)
        def _(j):
            gr, gi = grad_pair[j, 0], grad_pair[j, 1]
            for side, other in ((0, 1), (1, 0)):
                vr, vi = kb[b][pairs[j, other], 0], kb[b][pairs[j, other], 1]
                moved[side, j, 0] = vr * gr + vi * gi
                moved[side, j, 1] = vr * gi - vi * gr

        @pl.loop(0, M)
        def _(n):
            gr, gi = grads[b, n, 0], grads[b, n, 1]
            for j in range(J):
                for side, table in ((0, one_left), (1, one_right)):
                    w = table[j, n]
                    gr = gr + w * moved[side, j, 0]
                    gi = gi + w * moved[side, j, 1]
            grads[b, n, 0] = gr
            grads[b, n, 1] = gi

        for peer in mode_peers:
            go(grads.at[b, pl.ds(peer * ml, ml)], rows_back.at[b, me_m], gb_s.at[b, peer], gb_r.at[b, me_m], "mode", peer)
        own(("gb", b), grads.at[b, pl.ds(me_m * ml, ml)], rows_back.at[b, me_m])

    for b in range(Bl):
        owns[("gb", b)].wait()
        for peer in mode_peers:
            remote(
                grads.at[b, pl.ds(0, ml)], rows_back.at[b, peer], gb_s.at[b, peer], gb_r.at[b, peer], "mode", peer
            ).wait_recv()
        stacked = jnp.concatenate(
            [
                jnp.concatenate(
                    [
                        rows_back[b, i, m, ri, j * As : (j + 1) * As, :]
                        for ri in range(2)
                        for j in range(Dt)
                        for i in range(Dm)
                    ],
                    axis=0,
                )
                for m in range(ml)
            ],
            axis=1,
        )
        result = disperse(stacked, -1.0)
        for j in range(Dt):
            for ri in range(2):
                for m in range(ml):
                    row = ri * A + j * Al
                    send_out[j, b, ri, pl.ds(m, Al, stride=ml), :] = result[row : row + Al, m * 128 : (m + 1) * 128]
        for peer in tm_peers:
            go(send_out.at[peer, b], out.at[:, me_t * Bl + b], out_s.at[b, peer], out_r.at[b, me_t], "tm", peer)
        own(("out", b), send_out.at[me_t, b], out.at[:, me_t * Bl + b])
    for b in range(Bl):
        owns[("out", b)].wait()
        for peer in tm_peers:
            remote(
                send_out.at[0, b], out.at[:, peer * Bl + b], out_s.at[b, peer], out_r.at[b, peer], "tm", peer
            ).wait_recv()
    for copy in sends:
        copy.wait_send()


def on_device(Dm, Dt, input_field, target_field, margin, pair_index, mode_beta, segment_kind):
    _, B, ml, Tl = input_field.shape
    M, J = margin.shape[1], margin.shape[2]
    total = Tl * Dt
    A = total // 128
    Al = Tl // 128
    Bl = B // Dt
    As = Al // Dm
    Ak = As * Dt
    coeffs = lax.dynamic_index_in_dim(mode_beta, segment_kind[0], 0, keepdims=False)
    columns = lax.broadcasted_iota(jnp.int32, (J, M), 1)
    one_left = (pair_index[:, 0:1] == columns).astype(f32)
    one_right = (pair_index[:, 1:2] == columns).astype(f32)

    def by_rows(values):
        return values.reshape(2, B, ml, Al, 128).transpose(0, 1, 3, 2, 4).reshape(2, B, Al * ml, 128)

    x = by_rows(input_field)
    target = by_rows(target_field)
    if (As * ml) % 8:
        target = target.reshape(2, B, Dm, As * ml, 128).transpose(2, 0, 1, 3, 4)
    tables = make_tables(A, total)
    sizes = (Dt, Dm, B, Bl, ml, M, A, Al, As, Ak, J, total)
    vm = lambda *shape: pltpu.VMEM(shape, f32)
    dma = lambda *shape: pltpu.SemaphoreType.DMA(shape)
    anyspace = pl.BlockSpec(memory_space=pl.ANY)
    smem = pl.BlockSpec(memory_space=pltpu.SMEM)
    vmem = pl.BlockSpec(memory_space=pltpu.VMEM)
    out = pl.pallas_call(
        functools.partial(kernel, sizes),
        out_shape=jax.ShapeDtypeStruct((2, B, Al * ml, 128), f32),
        in_specs=[smem] * 4 + [anyspace, anyspace, vmem] + [anyspace] * 5,
        out_specs=vmem,
        scratch_shapes=[pltpu.VMEM(t.shape, bf16) for t in tables[:4]]
        + [
            vm(2, A, 128),
            vm(2, ml * A, 128),
            vm(Bl, Dt, 2, Al * ml, 128),
            vm(Dm, Bl, ml, 2, Ak, 128),
            [vm(M, 2, Ak, 128) for _ in range(Bl)],
            vm(Dm, 2, B, As * ml, 128),
            vm(Dt, Dm, 2, Bl, As * ml, 128),
            vm(Dm, ml, M * J),
            pltpu.SMEM((Dm, ml, M * J), f32),
            vm(J, 2, Ak, 128),
            vm(M * M, 2, Ak, 128),
            vm(J, 2, Ak, 128),
            vm(2, J, 2, Ak, 128),
            vm(M, 2, Ak, 128),
            vm(Bl, M, 2, Ak, 128),
            vm(Bl, Dm, ml, 2, Ak, 128),
            vm(Dt, Bl, 2, Al * ml, 128),
            dma(5),
            dma(4 * Bl + 4),
            dma(Bl, Dt), dma(Bl, Dt),
            dma(Dm), dma(Dm),
            dma(Dm), dma(Dm),
            dma(Dt), dma(Dt),
            dma(Bl, Dm), dma(Bl, Dm),
            dma(Bl, Dm), dma(Bl, Dm),
            dma(Bl, Dt), dma(Bl, Dt),
        ],
        compiler_params=pltpu.CompilerParams(collective_id=0, has_side_effects=True, vmem_limit_bytes=62 * 1024 * 1024),
    )(coeffs, pair_index, one_left, one_right, x, target, margin.reshape(ml, M * J), *[jnp.asarray(t) for t in tables])
    return out.reshape(2, B, Al, ml, 128).transpose(0, 1, 3, 2, 4).reshape(2, B, ml, Tl)


def solution(mesh):
    return jax.shard_map(
        functools.partial(on_device, mesh.shape["mode"], mesh.shape["tm"]),
        mesh=mesh,
        in_specs=(
            P(None, "dp", "mode", "tm"),
            P(None, "dp", "mode", "tm"),
            P("mode", None, None),
            P(),
            P(None, "mode", None),
            P(),
        ),
        out_specs=P(None, "dp", "mode", "tm"),
        check_vma=False,
    )
```

```python
import functools
import math

import jax
import jax.numpy as jnp
import numpy as np
from jax import lax
from jax.experimental import pallas as pl
from jax.experimental.pallas import tpu as pltpu
from jax.sharding import PartitionSpec as P

kerr_scale = 0.1
MESH = pl.DeviceIdType.MESH
f32 = jnp.float32
bf16 = jnp.bfloat16


def split_table(table):
    high = table.astype(np.float32).astype(bf16)
    low = (table - high.astype(np.float64)).astype(np.float32).astype(bf16)
    return np.stack([np.asarray(high), np.asarray(low)])


def real_form(size):
    turns = np.outer(np.arange(size), np.arange(size)) % size
    angle = turns * (2.0 * math.pi / size)
    cosine, sine = np.cos(angle), np.sin(angle)
    return np.block([[cosine, sine], [-sine, cosine]])


def make_tables(outer, total):
    left, right = real_form(outer), real_form(128)
    turns = np.outer(np.arange(outer), np.arange(128)) % total
    angle = turns * (2.0 * math.pi / total)
    twist = np.stack([np.cos(angle), -np.sin(angle)]).astype(np.float32)
    return (
        split_table(left),
        split_table(left.T / total),
        split_table(right.T),
        split_table(right),
        twist,
    )


def halves(value):
    high = value.astype(bf16)
    return high, (value - high.astype(f32)).astype(bf16)


def mm(a, b):
    return jnp.dot(a, b, preferred_element_type=f32)


def left_dot(table, value):
    high, low = halves(value)
    return mm(table[0], high) + (mm(table[0], low) + mm(table[1], high))


def right_dot(value, table):
    high, low = halves(value)
    return mm(high, table[0]) + (mm(low, table[0]) + mm(high, table[1]))


def farthest_first(me, count):
    low, high = jnp.int32(0), jnp.int32(count - 1)
    peers = []
    for _ in range(count - 1):
        up = (high - me >= me - low).astype(jnp.int32)
        peers.append(up * high + (1 - up) * low)
        high, low = high - up, low + 1 - up
    return peers


def kernel(
    sizes, kind, pairs, x, target, margin, beta_hbm,
    left_f_hbm, left_i_hbm, right_f_hbm, right_i_hbm, twist_hbm, out,
    left_f, left_i, right_f, right_i, twist, beta, phase_tab,
    rows_in, send_z, kb, t1, t2, mg, mg_s, prods, coup, grad_pair, moved, cots, grads, rows_back, send_out,
    table_sem, own_sem, in_s, in_r, mg_ss, mg_r, t1_s, t1_r, t2_s, t2_r, kb_s, kb_r, gb_s, gb_r, out_s, out_r,
):
    Dt, Dm, B, Bl, ml, M, A, Al, As, Ak, J, total = sizes
    me_t = lax.axis_index("tm")
    me_m = lax.axis_index("mode")
    tm_peers = farthest_first(me_t, Dt)
    mode_peers = farthest_first(me_m, Dm)

    def remote(src, dst, send, recv, axis, peer):
        return pltpu.make_async_remote_copy(
            src_ref=src, dst_ref=dst, send_sem=send, recv_sem=recv, device_id={axis: peer}, device_id_type=MESH
        )

    barrier = pltpu.get_barrier_semaphore()
    for peer in tm_peers:
        pl.semaphore_signal(barrier, inc=1, device_id={"tm": peer}, device_id_type=MESH)
    for peer in mode_peers:
        pl.semaphore_signal(barrier, inc=1, device_id={"mode": peer}, device_id_type=MESH)
    pl.semaphore_wait(barrier, Dt + Dm - 2)

    sends = []
    owns = {}
    own_count = [0]

    def go(src, dst, send, recv, axis, peer):
        copy = remote(src, dst, send, recv, axis, peer)
        copy.start()
        sends.append(copy)

    def own(name, src, dst):
        copy = pltpu.make_async_copy(src, dst, own_sem.at[own_count[0]])
        own_count[0] += 1
        copy.start()
        owns[name] = copy

    def target_part(i, b):
        if (As * ml) % 8 == 0:
            return target.at[:, :, b, pl.ds(pl.multiple_of(i * (As * ml), 8), As * ml), :]
        return target.at[i, :, :, b]

    def target_first_leg(b):
        for peer in mode_peers:
            go(target_part(peer, b), t1[b].at[me_m], t1_s.at[b, peer], t1_r.at[b, me_m], "mode", peer)
        own(("t1", b), target_part(me_m, b), t1[b].at[me_m])

    def target_second_leg(b):
        owns[("t1", b)].wait()
        for peer in mode_peers:
            remote(target_part(0, b), t1[b].at[peer], t1_s.at[b, peer], t1_r.at[b, peer], "mode", peer).wait_recv()
        for peer in tm_peers:
            go(t1[b].at[:, :, peer], t2[b].at[me_t], t2_s.at[b, peer], t2_r.at[b, me_t], "tm", peer)
        own(("t2", b), t1[b].at[:, :, me_t], t2[b].at[me_t])

    for b in range(Bl):
        for peer in tm_peers:
            go(x.at[:, peer * Bl + b], rows_in.at[b, me_t], in_s.at[b, peer], in_r.at[b, me_t], "tm", peer)
        own(("in", b), x.at[:, me_t * Bl + b], rows_in.at[b, me_t])
    for peer in mode_peers:
        go(margin, mg.at[me_m], mg_ss.at[peer], mg_r.at[me_m], "mode", peer)
    own("mg", margin, mg.at[me_m])
    target_first_leg(0)
    table_copies = []
    for spot, (src, dst) in enumerate(
        ((left_f_hbm, left_f), (left_i_hbm, left_i), (right_f_hbm, right_f), (right_i_hbm, right_i), (twist_hbm, twist), (beta_hbm, beta))
    ):
        copy = pltpu.make_async_copy(src, dst, table_sem.at[spot])
        copy.start()
        table_copies.append(copy)

    for copy in table_copies:
        copy.wait()
    low_digit = lax.broadcasted_iota(jnp.int32, (A, 128), 0)
    high_digit = lax.broadcasted_iota(jnp.int32, (A, 128), 1)
    frequency = low_digit + A * high_digit
    signed = jnp.where(frequency < total // 2, frequency, frequency - total).astype(f32)
    omega = signed * (8.0 / total)
    for m in range(ml):
        phase = (
            beta[0, m, kind[0]] * omega
            + beta[1, m, kind[0]] * (omega * omega) / 2.0
            + beta[2, m, kind[0]] * (omega * omega * omega) / 6.0
        )
        phase_tab[0, m * A : (m + 1) * A, :] = jnp.cos(phase)
        phase_tab[1, m * A : (m + 1) * A, :] = jnp.sin(phase)
    def disperse(stacked, direction):
        spun = left_dot(left_f, stacked)
        tw_r, tw_i = twist[0], twist[1]
        blocks = []
        for m in range(ml):
            re = spun[:A, m * 128 : (m + 1) * 128]
            im = spun[A:, m * 128 : (m + 1) * 128]
            blocks.append(jnp.concatenate([re * tw_r - im * tw_i, re * tw_i + im * tw_r], axis=1))
        spectrum = right_dot(jnp.concatenate(blocks, axis=0), right_f)
        re, im = spectrum[:, :128], spectrum[:, 128:]
        cosine = phase_tab[0]
        sine = phase_tab[1] * direction
        turned = jnp.concatenate([re * cosine - im * sine, re * sine + im * cosine], axis=1)
        back = right_dot(turned, right_i)
        real_rows, imag_rows = [], []
        for m in range(ml):
            re = back[m * A : (m + 1) * A, :128]
            im = back[m * A : (m + 1) * A, 128:]
            real_rows.append(re * tw_r + im * tw_i)
            imag_rows.append(im * tw_r - re * tw_i)
        joined = jnp.concatenate(
            [jnp.concatenate(real_rows, axis=1), jnp.concatenate(imag_rows, axis=1)], axis=0
        )
        return left_dot(left_i, joined)

    for b in range(Bl):
        owns[("in", b)].wait()
        for peer in tm_peers:
            remote(x.at[:, b], rows_in.at[b, peer], in_s.at[b, peer], in_r.at[b, peer], "tm", peer).wait_recv()
        stacked = jnp.concatenate(
            [
                jnp.concatenate(
                    [rows_in[b, j, ri, pl.ds(m, Al, stride=ml), :] for ri in range(2) for j in range(Dt)], axis=0
                )
                for m in range(ml)
            ],
            axis=1,
        )
        result = disperse(stacked, 1.0)
        for i in range(Dm):
            for m in range(ml):
                for ri in range(2):
                    for j in range(Dt):
                        row = ri * A + j * Al + i * As
                        send_z[i, b, m, ri, j * As : (j + 1) * As, :] = result[row : row + As, m * 128 : (m + 1) * 128]
        for peer in mode_peers:
            go(send_z.at[peer, b], kb[b].at[pl.ds(me_m * ml, ml)], kb_s.at[b, peer], kb_r.at[b, me_m], "mode", peer)
        own(("kb", b), send_z.at[me_m, b], kb[b].at[pl.ds(me_m * ml, ml)])
        if b + 1 < Bl:
            target_first_leg(b + 1)
        if b == 0:
            target_second_leg(0)

    owns["mg"].wait()
    for peer in mode_peers:
        remote(margin, mg.at[peer], mg_ss.at[peer], mg_r.at[peer], "mode", peer).wait_recv()
    own("mgs", mg, mg_s)
    owns["mgs"].wait()

    zero = jnp.zeros((Ak, 128), f32)

    def weight(p, n, j):
        return mg_s[p // ml, lax.rem(p, ml), n * J + j]

    for b in range(Bl):
        owns[("kb", b)].wait()
        for peer in mode_peers:
            remote(
                send_z.at[0, b], kb[b].at[pl.ds(peer * ml, ml)], kb_s.at[b, peer], kb_r.at[b, peer], "mode", peer
            ).wait_recv()
        owns[("t2", b)].wait()
        for peer in tm_peers:
            remote(t1[b].at[:, :, 0], t2[b].at[peer], t2_s.at[b, peer], t2_r.at[b, peer], "tm", peer).wait_recv()

        @pl.loop(0, J)
        def _(j):
            first, second = pairs[0, j], pairs[1, j]
            ar, ai = kb[b][first, 0], kb[b][first, 1]
            br, bi = kb[b][second, 0], kb[b][second, 1]
            prods[j, 0] = ar * br - ai * bi
            prods[j, 1] = ar * bi + ai * br

        @pl.loop(0, M)
        def _(p):
            def inner(step, carry):
                kr, ki = carry
                sums = [zero] * 4
                for j in range(J):
                    pr, pi = prods[j, 0], prods[j, 1]
                    for s in range(2):
                        w = weight(p, step * 2 + s, j)
                        sums[2 * s] = sums[2 * s] + w * pr
                        sums[2 * s + 1] = sums[2 * s + 1] + w * pi
                for s in range(2):
                    n = step * 2 + s
                    cr, ci = sums[2 * s], sums[2 * s + 1]
                    coup[p * M + n, 0] = cr
                    coup[p * M + n, 1] = ci
                    ur, ui = kb[b][n, 0], kb[b][n, 1]
                    kr = kr + (cr * ur + ci * ui)
                    ki = ki + (ci * ur - cr * ui)
                return kr, ki

            kr, ki = lax.fori_loop(0, M // 2, inner, (zero, zero))
            owner, local = p // ml, lax.rem(p, ml)
            wanted = [
                jnp.concatenate(
                    [t2[b][j, owner, ri, pl.ds(local, As, stride=ml), :] for j in range(Dt)], axis=0
                )
                for ri in range(2)
            ]
            cots[p, 0] = 2.0 * (kb[b][p, 0] - kerr_scale * ki - wanted[0])
            cots[p, 1] = 2.0 * (kb[b][p, 1] + kerr_scale * kr - wanted[1])

        @pl.loop(0, M)
        def _(n):
            ur, ui = kb[b][n, 0], kb[b][n, 1]

            def inner(p, carry):
                gr, gi = carry
                er, ei = kerr_scale * cots[p, 1], -kerr_scale * cots[p, 0]
                cr, ci = coup[p * M + n, 0], coup[p * M + n, 1]
                gr = gr + (er * cr + ei * ci)
                gi = gi + (er * ci - ei * cr)
                coup[p * M + n, 0] = er * ur - ei * ui
                coup[p * M + n, 1] = er * ui + ei * ur
                return gr, gi

            gr, gi = lax.fori_loop(0, M, inner, (cots[n, 0], cots[n, 1]))
            grads[b, n, 0] = gr
            grads[b, n, 1] = gi

        @pl.loop(0, J // 4)
        def _(quad):
            def outer(p, carry):
                sums = list(carry)
                for n in range(M):
                    sr, si = coup[p * M + n, 0], coup[p * M + n, 1]
                    for s in range(4):
                        w = weight(p, n, quad * 4 + s)
                        sums[2 * s] = sums[2 * s] + w * sr
                        sums[2 * s + 1] = sums[2 * s + 1] + w * si
                return tuple(sums)

            sums = lax.fori_loop(0, M, outer, (zero,) * 8)
            for s in range(4):
                grad_pair[quad * 4 + s, 0] = sums[2 * s]
                grad_pair[quad * 4 + s, 1] = sums[2 * s + 1]

        @pl.loop(0, J)
        def _(j):
            gr, gi = grad_pair[j, 0], grad_pair[j, 1]
            for side, other in ((0, 1), (1, 0)):
                vr, vi = kb[b][pairs[other, j], 0], kb[b][pairs[other, j], 1]
                moved[side, j, 0] = vr * gr + vi * gi
                moved[side, j, 1] = vr * gi - vi * gr

        @pl.loop(0, M)
        def _(n):
            gr, gi = grads[b, n, 0], grads[b, n, 1]
            for j in range(J):
                for side in range(2):
                    w = (pairs[side, j] == n).astype(f32)
                    gr = gr + w * moved[side, j, 0]
                    gi = gi + w * moved[side, j, 1]
            grads[b, n, 0] = gr
            grads[b, n, 1] = gi

        for peer in mode_peers:
            go(grads.at[b, pl.ds(peer * ml, ml)], rows_back.at[b, me_m], gb_s.at[b, peer], gb_r.at[b, me_m], "mode", peer)
        if b + 1 < Bl:
            target_second_leg(b + 1)
        own(("gb", b), grads.at[b, pl.ds(me_m * ml, ml)], rows_back.at[b, me_m])

    for b in range(Bl):
        owns[("gb", b)].wait()
        for peer in mode_peers:
            remote(
                grads.at[b, pl.ds(0, ml)], rows_back.at[b, peer], gb_s.at[b, peer], gb_r.at[b, peer], "mode", peer
            ).wait_recv()
        stacked = jnp.concatenate(
            [
                jnp.concatenate(
                    [
                        rows_back[b, i, m, ri, j * As : (j + 1) * As, :]
                        for ri in range(2)
                        for j in range(Dt)
                        for i in range(Dm)
                    ],
                    axis=0,
                )
                for m in range(ml)
            ],
            axis=1,
        )
        result = disperse(stacked, -1.0)
        for j in range(Dt):
            for ri in range(2):
                for m in range(ml):
                    row = ri * A + j * Al
                    send_out[j, b, ri, pl.ds(m, Al, stride=ml), :] = result[row : row + Al, m * 128 : (m + 1) * 128]
        for peer in tm_peers:
            go(send_out.at[peer, b], out.at[:, me_t * Bl + b], out_s.at[b, peer], out_r.at[b, me_t], "tm", peer)
        own(("out", b), send_out.at[me_t, b], out.at[:, me_t * Bl + b])
    for b in range(Bl):
        owns[("out", b)].wait()
        for peer in tm_peers:
            remote(
                send_out.at[0, b], out.at[:, peer * Bl + b], out_s.at[b, peer], out_r.at[b, peer], "tm", peer
            ).wait_recv()
    for copy in sends:
        copy.wait_send()


def on_device(Dm, Dt, input_field, target_field, margin, pair_index, mode_beta, segment_kind):
    _, B, ml, Tl = input_field.shape
    M, J = margin.shape[1], margin.shape[2]
    total = Tl * Dt
    A = total // 128
    Al = Tl // 128
    Bl = B // Dt
    As = Al // Dm
    Ak = As * Dt
    def by_rows(values):
        return values.reshape(2, B, ml, Al, 128).transpose(0, 1, 3, 2, 4).reshape(2, B, Al * ml, 128)

    x = by_rows(input_field)
    target = by_rows(target_field).reshape(2, Dt, Bl, Al * ml, 128)
    if (As * ml) % 8:
        target = target.reshape(2, Dt, Bl, Dm, As * ml, 128).transpose(3, 0, 1, 2, 4, 5)
    tables = make_tables(A, total)
    sizes = (Dt, Dm, B, Bl, ml, M, A, Al, As, Ak, J, total)
    vm = lambda *shape: pltpu.VMEM(shape, f32)
    dma = lambda *shape: pltpu.SemaphoreType.DMA(shape)
    anyspace = pl.BlockSpec(memory_space=pl.ANY)
    smem = pl.BlockSpec(memory_space=pltpu.SMEM)
    vmem = pl.BlockSpec(memory_space=pltpu.VMEM)
    out = pl.pallas_call(
        functools.partial(kernel, sizes),
        out_shape=jax.ShapeDtypeStruct((2, B, Al * ml, 128), f32),
        in_specs=[smem] * 2 + [anyspace, anyspace, vmem] + [anyspace] * 6,
        out_specs=vmem,
        scratch_shapes=[pltpu.VMEM(t.shape, bf16) for t in tables[:4]]
        + [
            vm(2, A, 128),
            pltpu.SMEM((3, ml, mode_beta.shape[0]), f32),
            vm(2, ml * A, 128),
            vm(Bl, Dt, 2, Al * ml, 128),
            vm(Dm, Bl, ml, 2, Ak, 128),
            [vm(M, 2, Ak, 128) for _ in range(Bl)],
            [vm(Dm, 2, Dt, As * ml, 128) for _ in range(Bl)],
            [vm(Dt, Dm, 2, As * ml, 128) for _ in range(Bl)],
            vm(Dm, ml, M * J),
            pltpu.SMEM((Dm, ml, M * J), f32),
            vm(J, 2, Ak, 128),
            vm(M * M, 2, Ak, 128),
            vm(J, 2, Ak, 128),
            vm(2, J, 2, Ak, 128),
            vm(M, 2, Ak, 128),
            vm(Bl, M, 2, Ak, 128),
            vm(Bl, Dm, ml, 2, Ak, 128),
            vm(Dt, Bl, 2, Al * ml, 128),
            dma(6),
            dma(6 * Bl + 2),
            dma(Bl, Dt), dma(Bl, Dt),
            dma(Dm), dma(Dm),
            dma(Bl, Dm), dma(Bl, Dm),
            dma(Bl, Dt), dma(Bl, Dt),
            dma(Bl, Dm), dma(Bl, Dm),
            dma(Bl, Dm), dma(Bl, Dm),
            dma(Bl, Dt), dma(Bl, Dt),
        ],
        compiler_params=pltpu.CompilerParams(collective_id=0, has_side_effects=True, vmem_limit_bytes=62 * 1024 * 1024),
    )(segment_kind, pair_index.T, x, target, margin.reshape(ml, M * J), mode_beta.transpose(2, 1, 0), *[jnp.asarray(t) for t in tables])
    return out.reshape(2, B, Al, ml, 128).transpose(0, 1, 3, 2, 4).reshape(2, B, ml, Tl)


def solution(mesh):
    return jax.shard_map(
        functools.partial(on_device, mesh.shape["mode"], mesh.shape["tm"]),
        mesh=mesh,
        in_specs=(
            P(None, "dp", "mode", "tm"),
            P(None, "dp", "mode", "tm"),
            P("mode", None, None),
            P(),
            P(None, "mode", None),
            P(),
        ),
        out_specs=P(None, "dp", "mode", "tm"),
        check_vma=False,
    )
```

```python
import functools
import math

import jax
import jax.numpy as jnp
import numpy as np
from jax import lax
from jax.experimental import pallas as pl
from jax.experimental.pallas import tpu as pltpu
from jax.sharding import PartitionSpec as P

kerr_scale = 0.1
MESH = pl.DeviceIdType.MESH
f32 = jnp.float32
bf16 = jnp.bfloat16


def split_table(table):
    high = table.astype(np.float32).astype(bf16)
    low = (table - high.astype(np.float64)).astype(np.float32).astype(bf16)
    return np.stack([np.asarray(high), np.asarray(low)])


def real_form(size):
    turns = np.outer(np.arange(size), np.arange(size)) % size
    angle = turns * (2.0 * math.pi / size)
    cosine, sine = np.cos(angle), np.sin(angle)
    return np.block([[cosine, sine], [-sine, cosine]])


def make_tables(outer, total):
    left, right = real_form(outer), real_form(128)
    turns = np.outer(np.arange(outer), np.arange(128)) % total
    angle = turns * (2.0 * math.pi / total)
    twist = np.stack([np.cos(angle), -np.sin(angle)]).astype(np.float32)
    return (
        split_table(left),
        split_table(left.T / total),
        split_table(right.T),
        split_table(right),
        twist,
    )


def halves(value):
    high = value.astype(bf16)
    return high, (value - high.astype(f32)).astype(bf16)


def mm(a, b):
    return jnp.dot(a, b, preferred_element_type=f32)


def left_dot(table, value):
    high, low = halves(value)
    return mm(table[0], high) + (mm(table[0], low) + mm(table[1], high))


def right_dot(value, table):
    high, low = halves(value)
    return mm(high, table[0]) + (mm(low, table[0]) + mm(high, table[1]))


def farthest_first(me, count):
    low, high = jnp.int32(0), jnp.int32(count - 1)
    peers = []
    for _ in range(count - 1):
        up = (high - me >= me - low).astype(jnp.int32)
        peers.append(up * high + (1 - up) * low)
        high, low = high - up, low + 1 - up
    return peers


def kernel(
    sizes, kind, pairs, x, target, margin, beta_hbm,
    left_f_hbm, left_i_hbm, right_f_hbm, right_i_hbm, twist_hbm, out,
    left_f, left_i, right_f, right_i, twist, beta, phase_tab,
    rows_in, send_z, kb, t1, t2, mg, mg_s, prods, coup, grad_pair, moved, cots, grads, rows_back, send_out,
    table_sem, own_sem, in_s, in_r, mg_ss, mg_r, t1_s, t1_r, t2_s, t2_r, kb_s, kb_r, gb_s, gb_r, out_s, out_r,
):
    Dt, Dm, B, Bl, ml, M, A, Al, As, Ak, J, total = sizes
    me_t = lax.axis_index("tm")
    me_m = lax.axis_index("mode")
    tm_peers = farthest_first(me_t, Dt)
    mode_peers = farthest_first(me_m, Dm)

    def remote(src, dst, send, recv, axis, peer):
        return pltpu.make_async_remote_copy(
            src_ref=src, dst_ref=dst, send_sem=send, recv_sem=recv, device_id={axis: peer}, device_id_type=MESH
        )

    barrier = pltpu.get_barrier_semaphore()
    for peer in tm_peers:
        pl.semaphore_signal(barrier, inc=1, device_id={"tm": peer}, device_id_type=MESH)
    for peer in mode_peers:
        pl.semaphore_signal(barrier, inc=1, device_id={"mode": peer}, device_id_type=MESH)
    pl.semaphore_wait(barrier, Dt + Dm - 2)

    sends = []
    owns = {}
    own_count = [0]

    def go(src, dst, send, recv, axis, peer):
        copy = remote(src, dst, send, recv, axis, peer)
        copy.start()
        sends.append(copy)

    def own(name, src, dst):
        copy = pltpu.make_async_copy(src, dst, own_sem.at[own_count[0]])
        own_count[0] += 1
        copy.start()
        owns[name] = copy

    def target_part(i, b):
        if (As * ml) % 8 == 0:
            return target.at[:, :, b, pl.ds(pl.multiple_of(i * (As * ml), 8), As * ml), :]
        return target.at[i, :, :, b]

    def target_first_leg(b):
        for peer in mode_peers:
            go(target_part(peer, b), t1[b].at[me_m], t1_s.at[b, peer], t1_r.at[b, me_m], "mode", peer)
        own(("t1", b), target_part(me_m, b), t1[b].at[me_m])

    def target_second_leg(b):
        owns[("t1", b)].wait()
        for peer in mode_peers:
            remote(target_part(0, b), t1[b].at[peer], t1_s.at[b, peer], t1_r.at[b, peer], "mode", peer).wait_recv()
        for peer in tm_peers:
            go(t1[b].at[:, :, peer], t2[b].at[me_t], t2_s.at[b, peer], t2_r.at[b, me_t], "tm", peer)
        own(("t2", b), t1[b].at[:, :, me_t], t2[b].at[me_t])

    for b in range(Bl):
        for peer in tm_peers:
            go(x.at[:, peer * Bl + b], rows_in.at[b, me_t], in_s.at[b, peer], in_r.at[b, me_t], "tm", peer)
        own(("in", b), x.at[:, me_t * Bl + b], rows_in.at[b, me_t])
    for peer in mode_peers:
        go(margin, mg.at[me_m], mg_ss.at[peer], mg_r.at[me_m], "mode", peer)
    own("mg", margin, mg.at[me_m])
    target_first_leg(0)
    table_copies = []
    for spot, (src, dst) in enumerate(
        ((left_f_hbm, left_f), (left_i_hbm, left_i), (right_f_hbm, right_f), (right_i_hbm, right_i), (twist_hbm, twist), (beta_hbm, beta))
    ):
        copy = pltpu.make_async_copy(src, dst, table_sem.at[spot])
        copy.start()
        table_copies.append(copy)

    for copy in table_copies:
        copy.wait()
    low_digit = lax.broadcasted_iota(jnp.int32, (A, 128), 0)
    high_digit = lax.broadcasted_iota(jnp.int32, (A, 128), 1)
    frequency = low_digit + A * high_digit
    signed = jnp.where(frequency < total // 2, frequency, frequency - total).astype(f32)
    omega = signed * (8.0 / total)
    for m in range(ml):
        phase = (
            beta[0, m, kind[0]] * omega
            + beta[1, m, kind[0]] * (omega * omega) / 2.0
            + beta[2, m, kind[0]] * (omega * omega * omega) / 6.0
        )
        phase_tab[0, m * A : (m + 1) * A, :] = jnp.cos(phase)
        phase_tab[1, m * A : (m + 1) * A, :] = jnp.sin(phase)
    def disperse(stacked, direction):
        spun = left_dot(left_f, stacked)
        tw_r, tw_i = twist[0], twist[1]
        blocks = []
        for m in range(ml):
            re = spun[:A, m * 128 : (m + 1) * 128]
            im = spun[A:, m * 128 : (m + 1) * 128]
            blocks.append(jnp.concatenate([re * tw_r - im * tw_i, re * tw_i + im * tw_r], axis=1))
        spectrum = right_dot(jnp.concatenate(blocks, axis=0), right_f)
        re, im = spectrum[:, :128], spectrum[:, 128:]
        cosine = phase_tab[0]
        sine = phase_tab[1] * direction
        turned = jnp.concatenate([re * cosine - im * sine, re * sine + im * cosine], axis=1)
        back = right_dot(turned, right_i)
        real_rows, imag_rows = [], []
        for m in range(ml):
            re = back[m * A : (m + 1) * A, :128]
            im = back[m * A : (m + 1) * A, 128:]
            real_rows.append(re * tw_r + im * tw_i)
            imag_rows.append(im * tw_r - re * tw_i)
        joined = jnp.concatenate(
            [jnp.concatenate(real_rows, axis=1), jnp.concatenate(imag_rows, axis=1)], axis=0
        )
        return left_dot(left_i, joined)

    for b in range(Bl):
        owns[("in", b)].wait()
        for peer in tm_peers:
            remote(x.at[:, b], rows_in.at[b, peer], in_s.at[b, peer], in_r.at[b, peer], "tm", peer).wait_recv()
        stacked = jnp.concatenate(
            [
                jnp.concatenate(
                    [rows_in[b, j, ri, pl.ds(m, Al, stride=ml), :] for ri in range(2) for j in range(Dt)], axis=0
                )
                for m in range(ml)
            ],
            axis=1,
        )
        result = disperse(stacked, 1.0)
        for i in range(Dm):
            for m in range(ml):
                for ri in range(2):
                    for j in range(Dt):
                        row = ri * A + j * Al + i * As
                        send_z[i, b, m, ri, j * As : (j + 1) * As, :] = result[row : row + As, m * 128 : (m + 1) * 128]
        for peer in mode_peers:
            go(send_z.at[peer, b], kb[b].at[pl.ds(me_m * ml, ml)], kb_s.at[b, peer], kb_r.at[b, me_m], "mode", peer)
        own(("kb", b), send_z.at[me_m, b], kb[b].at[pl.ds(me_m * ml, ml)])
        if b + 1 < Bl:
            target_first_leg(b + 1)
        if b == 0:
            target_second_leg(0)

    owns["mg"].wait()
    for peer in mode_peers:
        remote(margin, mg.at[peer], mg_ss.at[peer], mg_r.at[peer], "mode", peer).wait_recv()
    own("mgs", mg, mg_s)
    owns["mgs"].wait()

    zero = jnp.zeros((Ak, 128), f32)

    def weight(p, n, j):
        return mg_s[p // ml, lax.rem(p, ml), n * J + j]

    for b in range(Bl):
        owns[("kb", b)].wait()
        for peer in mode_peers:
            remote(
                send_z.at[0, b], kb[b].at[pl.ds(peer * ml, ml)], kb_s.at[b, peer], kb_r.at[b, peer], "mode", peer
            ).wait_recv()
        owns[("t2", b)].wait()
        for peer in tm_peers:
            remote(t1[b].at[:, :, 0], t2[b].at[peer], t2_s.at[b, peer], t2_r.at[b, peer], "tm", peer).wait_recv()

        @pl.loop(0, J)
        def _(j):
            first, second = pairs[0, j], pairs[1, j]
            ar, ai = kb[b][first, 0], kb[b][first, 1]
            br, bi = kb[b][second, 0], kb[b][second, 1]
            prods[j, 0] = ar * br - ai * bi
            prods[j, 1] = ar * bi + ai * br

        @pl.loop(0, M)
        def _(p):
            def inner(step, carry):
                kr, ki = carry
                sums = [zero] * 4
                for j in range(J):
                    pr, pi = prods[j, 0], prods[j, 1]
                    for s in range(2):
                        w = weight(p, step * 2 + s, j)
                        sums[2 * s] = sums[2 * s] + w * pr
                        sums[2 * s + 1] = sums[2 * s + 1] + w * pi
                for s in range(2):
                    n = step * 2 + s
                    cr, ci = sums[2 * s], sums[2 * s + 1]
                    coup[p * M + n, 0] = cr
                    coup[p * M + n, 1] = ci
                    ur, ui = kb[b][n, 0], kb[b][n, 1]
                    kr = kr + (cr * ur + ci * ui)
                    ki = ki + (ci * ur - cr * ui)
                return kr, ki

            kr, ki = lax.fori_loop(0, M // 2, inner, (zero, zero), unroll=4)
            owner, local = p // ml, lax.rem(p, ml)
            wanted = [
                jnp.concatenate(
                    [t2[b][j, owner, ri, pl.ds(local, As, stride=ml), :] for j in range(Dt)], axis=0
                )
                for ri in range(2)
            ]
            cots[p, 0] = 2.0 * (kb[b][p, 0] - kerr_scale * ki - wanted[0])
            cots[p, 1] = 2.0 * (kb[b][p, 1] + kerr_scale * kr - wanted[1])

        @pl.loop(0, M)
        def _(n):
            ur, ui = kb[b][n, 0], kb[b][n, 1]

            def inner(p, carry):
                gr, gi = carry
                er, ei = kerr_scale * cots[p, 1], -kerr_scale * cots[p, 0]
                cr, ci = coup[p * M + n, 0], coup[p * M + n, 1]
                gr = gr + (er * cr + ei * ci)
                gi = gi + (er * ci - ei * cr)
                coup[p * M + n, 0] = er * ur - ei * ui
                coup[p * M + n, 1] = er * ui + ei * ur
                return gr, gi

            gr, gi = lax.fori_loop(0, M, inner, (cots[n, 0], cots[n, 1]), unroll=8)
            grads[b, n, 0] = gr
            grads[b, n, 1] = gi

        @pl.loop(0, J // 4)
        def _(quad):
            def outer(p, carry):
                sums = list(carry)
                for n in range(M):
                    sr, si = coup[p * M + n, 0], coup[p * M + n, 1]
                    for s in range(4):
                        w = weight(p, n, quad * 4 + s)
                        sums[2 * s] = sums[2 * s] + w * sr
                        sums[2 * s + 1] = sums[2 * s + 1] + w * si
                return tuple(sums)

            sums = lax.fori_loop(0, M, outer, (zero,) * 8)
            for s in range(4):
                grad_pair[quad * 4 + s, 0] = sums[2 * s]
                grad_pair[quad * 4 + s, 1] = sums[2 * s + 1]

        @pl.loop(0, J)
        def _(j):
            gr, gi = grad_pair[j, 0], grad_pair[j, 1]
            for side, other in ((0, 1), (1, 0)):
                vr, vi = kb[b][pairs[other, j], 0], kb[b][pairs[other, j], 1]
                moved[side, j, 0] = vr * gr + vi * gi
                moved[side, j, 1] = vr * gi - vi * gr

        @pl.loop(0, M)
        def _(n):
            gr, gi = grads[b, n, 0], grads[b, n, 1]
            for j in range(J):
                for side in range(2):
                    w = (pairs[side, j] == n).astype(f32)
                    gr = gr + w * moved[side, j, 0]
                    gi = gi + w * moved[side, j, 1]
            grads[b, n, 0] = gr
            grads[b, n, 1] = gi

        for peer in mode_peers:
            go(grads.at[b, pl.ds(peer * ml, ml)], rows_back.at[b, me_m], gb_s.at[b, peer], gb_r.at[b, me_m], "mode", peer)
        if b + 1 < Bl:
            target_second_leg(b + 1)
        own(("gb", b), grads.at[b, pl.ds(me_m * ml, ml)], rows_back.at[b, me_m])

    for b in range(Bl):
        owns[("gb", b)].wait()
        for peer in mode_peers:
            remote(
                grads.at[b, pl.ds(0, ml)], rows_back.at[b, peer], gb_s.at[b, peer], gb_r.at[b, peer], "mode", peer
            ).wait_recv()
        stacked = jnp.concatenate(
            [
                jnp.concatenate(
                    [
                        rows_back[b, i, m, ri, j * As : (j + 1) * As, :]
                        for ri in range(2)
                        for j in range(Dt)
                        for i in range(Dm)
                    ],
                    axis=0,
                )
                for m in range(ml)
            ],
            axis=1,
        )
        result = disperse(stacked, -1.0)
        for j in range(Dt):
            for ri in range(2):
                for m in range(ml):
                    row = ri * A + j * Al
                    send_out[j, b, ri, pl.ds(m, Al, stride=ml), :] = result[row : row + Al, m * 128 : (m + 1) * 128]
        for peer in tm_peers:
            go(send_out.at[peer, b], out.at[:, me_t * Bl + b], out_s.at[b, peer], out_r.at[b, me_t], "tm", peer)
        own(("out", b), send_out.at[me_t, b], out.at[:, me_t * Bl + b])
    for b in range(Bl):
        owns[("out", b)].wait()
        for peer in tm_peers:
            remote(
                send_out.at[0, b], out.at[:, peer * Bl + b], out_s.at[b, peer], out_r.at[b, peer], "tm", peer
            ).wait_recv()
    for copy in sends:
        copy.wait_send()


def on_device(Dm, Dt, input_field, target_field, margin, pair_index, mode_beta, segment_kind):
    _, B, ml, Tl = input_field.shape
    M, J = margin.shape[1], margin.shape[2]
    total = Tl * Dt
    A = total // 128
    Al = Tl // 128
    Bl = B // Dt
    As = Al // Dm
    Ak = As * Dt
    def by_rows(values):
        return values.reshape(2, B, ml, Al, 128).transpose(0, 1, 3, 2, 4).reshape(2, B, Al * ml, 128)

    x = by_rows(input_field)
    target = by_rows(target_field).reshape(2, Dt, Bl, Al * ml, 128)
    if (As * ml) % 8:
        target = target.reshape(2, Dt, Bl, Dm, As * ml, 128).transpose(3, 0, 1, 2, 4, 5)
    tables = make_tables(A, total)
    sizes = (Dt, Dm, B, Bl, ml, M, A, Al, As, Ak, J, total)
    vm = lambda *shape: pltpu.VMEM(shape, f32)
    dma = lambda *shape: pltpu.SemaphoreType.DMA(shape)
    anyspace = pl.BlockSpec(memory_space=pl.ANY)
    smem = pl.BlockSpec(memory_space=pltpu.SMEM)
    vmem = pl.BlockSpec(memory_space=pltpu.VMEM)
    out = pl.pallas_call(
        functools.partial(kernel, sizes),
        out_shape=jax.ShapeDtypeStruct((2, B, Al * ml, 128), f32),
        in_specs=[smem] * 2 + [anyspace, anyspace, vmem] + [anyspace] * 6,
        out_specs=vmem,
        scratch_shapes=[pltpu.VMEM(t.shape, bf16) for t in tables[:4]]
        + [
            vm(2, A, 128),
            pltpu.SMEM((3, ml, mode_beta.shape[0]), f32),
            vm(2, ml * A, 128),
            vm(Bl, Dt, 2, Al * ml, 128),
            vm(Dm, Bl, ml, 2, Ak, 128),
            [vm(M, 2, Ak, 128) for _ in range(Bl)],
            [vm(Dm, 2, Dt, As * ml, 128) for _ in range(Bl)],
            [vm(Dt, Dm, 2, As * ml, 128) for _ in range(Bl)],
            vm(Dm, ml, M * J),
            pltpu.SMEM((Dm, ml, M * J), f32),
            vm(J, 2, Ak, 128),
            vm(M * M, 2, Ak, 128),
            vm(J, 2, Ak, 128),
            vm(2, J, 2, Ak, 128),
            vm(M, 2, Ak, 128),
            vm(Bl, M, 2, Ak, 128),
            vm(Bl, Dm, ml, 2, Ak, 128),
            vm(Dt, Bl, 2, Al * ml, 128),
            dma(6),
            dma(6 * Bl + 2),
            dma(Bl, Dt), dma(Bl, Dt),
            dma(Dm), dma(Dm),
            dma(Bl, Dm), dma(Bl, Dm),
            dma(Bl, Dt), dma(Bl, Dt),
            dma(Bl, Dm), dma(Bl, Dm),
            dma(Bl, Dm), dma(Bl, Dm),
            dma(Bl, Dt), dma(Bl, Dt),
        ],
        compiler_params=pltpu.CompilerParams(collective_id=0, has_side_effects=True, vmem_limit_bytes=62 * 1024 * 1024),
    )(segment_kind, pair_index.T, x, target, margin.reshape(ml, M * J), mode_beta.transpose(2, 1, 0), *[jnp.asarray(t) for t in tables])
    return out.reshape(2, B, Al, ml, 128).transpose(0, 1, 3, 2, 4).reshape(2, B, ml, Tl)


def solution(mesh):
    return jax.shard_map(
        functools.partial(on_device, mesh.shape["mode"], mesh.shape["tm"]),
        mesh=mesh,
        in_specs=(
            P(None, "dp", "mode", "tm"),
            P(None, "dp", "mode", "tm"),
            P("mode", None, None),
            P(),
            P(None, "mode", None),
            P(),
        ),
        out_specs=P(None, "dp", "mode", "tm"),
        check_vma=False,
    )
```
